32 devices in a mesh: mom: 4 (over y, core), tm: 4 (over z), pt: 2 (over x).
Axes of the slice: x: 2, y: 2, z: 4, core: 2. Of those that a mesh axis runs over, the one named last changes fastest.
Arguments:
- chi_time: bfloat16 [16, 8, 896, 896], P('tm', 'mom', 'pt'), may hold values from -4 to 4
- green: bfloat16 [8, 16, 896, 896], P('mom', 'tm', 'pt'), may hold values from -6 to 6
- band_coeffs: bfloat16 [896, 1024], replicated, may hold values from -1 to 1
Outputs:
- self_energy: float32 [8, 16, 1024], P('mom', 'tm', 'pt')
The draws below stay inside these ranges and needn't reach their ends.
All inputs are finite; a program needn't handle non-finite values.
Results may differ from the reference program's by a relative error of at most 0.009.
Values may be sent and summed in bfloat16 or wider, within the bound.
A program may use at most 128 MiB of HBM per device.

```python
import math
import jax
import jax.numpy as jnp
from jax import lax

NK = 8
NT = 16
NP = 896
NB = 1024
ORDER = 8


def draw_chi_time(key, part):
    shape = (NT, NK, NP, NP)
    values = jnp.clip(jax.random.normal(key, shape, jnp.float32), -4.0, 4.0)
    return values.astype(jnp.bfloat16)


def block_scale(key, extent, cuts, low, largest):
    level, own = 1.0, jax.random.fold_in(key, 6)
    for position, parts in cuts:
        draws = jnp.exp(jax.random.uniform(jax.random.fold_in(own, position), (parts,), jnp.float32, low / len(cuts), largest / len(cuts)))
        level = level * jnp.repeat(draws, extent[position] // parts).reshape([-1 if axis == position else 1 for axis in range(len(extent))])
    return level


def bell_draw(key, shape, deviation, bound, pieces=(), kind=jnp.bfloat16):
    entries = deviation * jax.random.normal(key, shape, jnp.float32)
    if pieces:
        entries = entries * block_scale(key, shape, pieces, -0.22, 0.18)
    return jnp.clip(entries, -bound, bound).astype(kind)


def setup_inputs(seed: int = 0) -> dict:
    keys = jax.random.split(jax.random.key(seed), 4)
    return {
        "chi_time": draw_chi_time(jax.random.fold_in(keys[3], 71), 0),
        "green": bell_draw(keys[1], (NK, NT, NP, NP), 1.0, 6.0, ((0, 4), (1, 4), (2, 2))),
        "band_coeffs": bell_draw(keys[2], (NP, NB), 28 ** -0.5, 1.0),
    }


COUPLING = 0.8

def cosine_table(count):
    index = jnp.arange(count, dtype=jnp.float32) + 0.5
    angle = jnp.pi * index[:, None] * index[None, :] / count
    return (jnp.sqrt(jnp.float32(2.0 / count)) * jnp.cos(angle)).astype(jnp.bfloat16)

def hartley_table(count):
    index = jnp.arange(count, dtype=jnp.float32)
    angle = 2.0 * jnp.pi * index[:, None] * index[None, :] / count
    return (jnp.cos(angle) + jnp.sin(angle)) / jnp.sqrt(jnp.float32(count))

def series_tile(tile):
    power = tile
    total = tile.astype(jnp.float32)
    for term in range(ORDER - 1):
        power = jnp.dot(power, tile, preferred_element_type=jnp.float32).astype(jnp.bfloat16)
        total = total + power.astype(jnp.float32)
    return total.astype(jnp.bfloat16)

def reference(chi_time, green, band_coeffs):
    highest = lax.Precision.HIGHEST
    cosine = cosine_table(NT).astype(jnp.float32)
    hartley = hartley_table(NK)
    scale = COUPLING / math.sqrt(NP)
    freq = jnp.einsum('wt,tkpq->wkpq', cosine, chi_time.astype(jnp.float32), precision=highest)
    freq = (scale * freq).astype(jnp.bfloat16)
    screened = lax.map(series_tile, freq.reshape(NT * NK, NP, NP)).reshape(NT, NK, NP, NP)
    timed = jnp.einsum('tw,wkpq->tkpq', cosine, screened.astype(jnp.float32), precision=highest)
    lattice = jnp.einsum('rk,tkpq->rtpq', hartley, timed, precision=highest)
    sigma = (green.astype(jnp.float32) * lattice).astype(jnp.bfloat16)
    coeffs = band_coeffs.astype(jnp.float32)

    def project(tile):
        applied = jnp.dot(tile, band_coeffs, preferred_element_type=jnp.float32)
        return lax.optimization_barrier(jnp.sum(coeffs * applied, axis=0))
    values = lax.map(project, sigma.reshape(NK * NT, NP, NP))
    return values.reshape(NK, NT, NB)
```

```python
import functools
import math

import jax
import jax.numpy as jnp
import numpy as np
from jax import lax
from jax.experimental import pallas as pl
from jax.experimental.pallas import tpu as pltpu
from jax.sharding import PartitionSpec as P

COUPLING = 0.8
MESH = pl.DeviceIdType.MESH
BF16, F32 = jnp.bfloat16, jnp.float32


def cosine_table(count):
    index = np.arange(count, dtype=np.float64) + 0.5
    angle = np.pi * index[:, None] * index[None, :] / count
    return (np.sqrt(2.0 / count) * np.cos(angle)).astype(np.float32).astype(BF16)


def hartley_table(count):
    index = np.arange(count, dtype=np.float64)
    angle = 2.0 * np.pi * index[:, None] * index[None, :] / count
    return ((np.cos(angle) + np.sin(angle)) / np.sqrt(count)).astype(np.float32).astype(BF16)


def spread_table(table, rows):
    return jnp.asarray(np.kron(table.astype(np.float32), np.eye(rows, dtype=np.float32)).astype(BF16))


def group_rows(rows, largest):
    size = largest
    while rows % size:
        size //= 2
    return size


def flip(index, bits, count):
    total, place = 0, 1
    while place < count:
        bit = (index // place) % 2
        total = total + place * ((1 - bit) if (bits // place) % 2 else bit)
        place *= 2
    return total


def stacked(value):
    count, rows, width = value.shape
    if rows % 16:
        return value.astype(F32).reshape(count * rows, width).astype(BF16)
    return value.reshape(count * rows, width)


def dot(left, right):
    return jnp.dot(left, right, preferred_element_type=F32)


def kernel(dims, chi, green, band, mixer, turner, out, raw, mix, tiles, four, fourth, square, lat,
           cells, total, part, gathered, send1, recv1, send_g, recv_g, send2, recv2, send3, recv3,
           send4, recv4, send6, recv6):
    mom, tm, pt, times_dev, moms_dev, rows_dev, points, low, half, own_w, size1, size3, group, group_h = dims
    m, z, x = lax.axis_index("mom"), lax.axis_index("tm"), lax.axis_index("pt")
    ml, mh = m % low, m // low
    fan = pt * low
    seat = x * low + ml
    count_t = times_dev * tm
    chunks1, chunks3 = half // size1, half // size3
    scale = COUPLING / math.sqrt(points)

    def remote(source, target, send, recv, where):
        return pltpu.make_async_remote_copy(
            src_ref=source, dst_ref=target, send_sem=send, recv_sem=recv,
            device_id=dict(zip(("mom", "tm", "pt"), where)), device_id_type=MESH)

    def await_bytes(ref, sem):
        pltpu.make_async_copy(ref, ref, sem).wait()

    def rows(start, size):
        return pl.ds(pl.multiple_of(start, size), size)

    barrier = pltpu.get_barrier_semaphore()
    greeted = 0
    for i in range(mom):
        for j in range(tm):
            if i or j:
                pl.semaphore_signal(barrier, inc=1, device_id={
                    "mom": flip(m, i, mom), "tm": flip(z, j, tm), "pt": x}, device_id_type=MESH)
                greeted += 1
        for a in range(1, pt):
            pl.semaphore_signal(barrier, inc=1, device_id={
                "mom": flip(m, i, mom), "tm": z, "pt": flip(x, a, pt)}, device_id_type=MESH)
            greeted += 1
    pl.semaphore_wait(barrier, greeted)

    @pl.loop(0, chunks1)
    def _(c):
        for kl in range(moms_dev):
            to_z = moms_dev * ml + kl
            for b in range(low):
                to_l = flip(ml, b, low)
                source = chi.at[:, kl, rows(to_l * half + c * size1, size1), :]
                target = raw.at[pl.ds(times_dev * z, times_dev), rows(c * size1, size1), :]
                move = remote(source, target, send1, recv1.at[c], (mh * low + to_l, to_z, x))
                if b:
                    move.start()
                else:
                    here = to_z == z

                    @pl.when(here)
                    def _():
                        pltpu.make_async_copy(source, target, recv1.at[c]).start()

                    @pl.when(jnp.logical_not(here))
                    def _():
                        move.start()

    for i in range(mom):
        to_m = flip(m, i, mom)
        source = green.at[:, to_m]
        target = cells.at[pl.ds(moms_dev * m, moms_dev)]
        if i:
            remote(source, target, send_g, recv_g, (to_m, z, x)).start()
        else:
            pltpu.make_async_copy(source, target, recv_g).start()

    @pl.loop(0, chunks1)
    def _(c):
        await_bytes(raw.at[:, rows(c * size1, size1), :], recv1.at[c])

        @pl.loop(0, size1 // group)
        def _(g):
            block = rows(c * size1 + g * group, group)
            mixed = scale * dot(mixer[...], stacked(raw[:, block, :]))
            mix[:, block, :] = mixed.reshape(count_t, group, points).astype(BF16)

        for a in reversed(range(pt)):
            for b in range(low):
                to_x, to_l = flip(x, a, pt), flip(ml, b, low)
                source = mix.at[pl.ds(own_w * (to_x * low + to_l), own_w), rows(c * size1, size1), :]
                target = tiles.at[:, rows(seat * half + c * size1, size1), :]
                if a or b:
                    remote(source, target, send2, recv2, (mh * low + to_l, z, to_x)).start()
                else:
                    pltpu.make_async_copy(source, target, recv2).start()

    await_bytes(tiles, recv2)

    step = points
    while step > 256:
        step //= 2

    @pl.loop(0, own_w)
    def _(w):
        @pl.loop(0, points // step)
        def _(r):
            block = rows(r * step, step)
            square[block, :] = dot(tiles[w, block, :], tiles[w]).astype(BF16)

        @pl.loop(0, points // step)
        def _(r):
            block = rows(r * step, step)
            second = square[block, :]
            two = (tiles[w, block, :].astype(F32) + second.astype(F32)).astype(BF16)
            both = dot(jnp.concatenate([second, two], axis=0), square[...])
            fourth[w, block, :] = both[:step].astype(BF16)
            four[w, block, :] = (two.astype(F32) + both[step:]).astype(BF16)

    @pl.loop(0, chunks3)
    def _(c):
        @pl.loop(0, own_w)
        def _(w):
            if chunks3 == 1:
                left = four[w]
                tiles[w] = (left.astype(F32) + dot(left, fourth[w])).astype(BF16)
            else:
                places = [rows(d * half + c * size3, size3) for d in range(fan)]
                left = jnp.concatenate([four[w, place, :] for place in places], axis=0)
                last = (left.astype(F32) + dot(left, fourth[w])).astype(BF16)
                for d, place in enumerate(places):
                    tiles[w, place, :] = last[d * size3:(d + 1) * size3]

        for a in reversed(range(pt)):
            for b in range(low):
                to_x, to_l = flip(x, a, pt), flip(ml, b, low)
                source = tiles.at[:, rows((to_x * low + to_l) * half + c * size3, size3), :]
                target = raw.at[pl.ds(own_w * seat, own_w), rows(c * size3, size3), :]
                if a or b:
                    remote(source, target, send3, recv3.at[c], (mh * low + to_l, z, to_x)).start()
                else:
                    pltpu.make_async_copy(source, target, recv3.at[c]).start()

    await_bytes(mix.at[pl.ds(0, count_t - own_w)], send2)

    @pl.loop(0, chunks3)
    def _(c):
        await_bytes(raw.at[:, rows(c * size3, size3), :], recv3.at[c])

        @pl.loop(0, size3 // group)
        def _(g):
            block = rows(c * size3 + g * group, group)
            timed = dot(mixer[...], stacked(raw[:, block, :]))
            mix[:, block, :] = timed.reshape(count_t, group, points).astype(BF16)

        for j in reversed(range(tm)):
            for i in range(mom):
                to_m, to_z = flip(m, i, mom), flip(z, j, tm)
                source = mix.at[times_dev * to_z + to_m, rows(c * size3, size3), :]
                target = lat.at[tm * mh + z, ml, rows(c * size3, size3), :]
                if i or j:
                    remote(source, target, send4, recv4.at[c], (to_m, to_z, x)).start()
                else:
                    pltpu.make_async_copy(source, target, recv4.at[c]).start()

    await_bytes(cells, recv_g)
    total[...] = jnp.zeros_like(total)
    count_k = moms_dev * mom
    bands = band.shape[1]

    @pl.loop(0, chunks3)
    def _(c):
        await_bytes(lat.at[:, :, rows(c * size3, size3), :], recv4.at[c])
        for side in range(low):
            @pl.loop(0, size3 // group_h)
            def _(g):
                block = rows(c * size3 + g * group_h, group_h)
                place = rows(side * half + c * size3 + g * group_h, group_h)
                own = rows(x * rows_dev + side * half + c * size3 + g * group_h, group_h)
                lattice = dot(turner[...], stacked(lat[:, side, block, :]))
                lattice = lattice.reshape(count_k, group_h, points)
                sigma = (cells[:, place, :].astype(F32) * lattice).astype(BF16)
                applied = dot(stacked(sigma), band[...])
                applied = applied.reshape(count_k, group_h, bands) * band[own, :].astype(F32)[None]
                total[...] += jnp.sum(applied.reshape(count_k, group_h // 8, 8, bands), axis=1)

    share = bands // pt
    for to_m in range(mom):
        for to_x in range(pt):
            value = total[pl.ds(moms_dev * to_m, moms_dev), :, pl.ds(to_x * share, share)]
            part[to_m * pt + to_x] = jnp.sum(value, axis=1)
    for i in range(mom):
        for a in range(pt):
            to_m, to_x = flip(m, i, mom), flip(x, a, pt)
            source, target = part.at[to_m * pt + to_x], gathered.at[m * pt + x]
            if i or a:
                remote(source, target, send6, recv6, (to_m, z, to_x)).start()
            else:
                pltpu.make_async_copy(source, target, recv6).start()
    await_bytes(gathered, recv6)
    for t in range(times_dev):
        value = gathered[t * pt]
        for a in range(1, pt):
            value = value + gathered[t * pt + a]
        out[:, t, :] = value

    stays = z // moms_dev == ml

    @pl.when(stays)
    def _():
        await_bytes(chi.at[pl.ds(0, times_dev - times_dev // (low * moms_dev))], send1)

    @pl.when(jnp.logical_not(stays))
    def _():
        await_bytes(chi, send1)

    await_bytes(green.at[:, pl.ds(0, mom - 1)], send_g)
    await_bytes(mix.at[pl.ds(0, count_t - own_w)], send3)
    await_bytes(mix.at[pl.ds(0, count_t - 1)], send4)
    await_bytes(part.at[pl.ds(0, mom * pt - 1)], send6)


def local(mom, tm, pt, chi, green, band):
    times_dev, moms_dev, rows_dev, points = chi.shape
    bands = band.shape[1]
    count_t, count_k = times_dev * tm, moms_dev * mom
    low = tm // moms_dev
    half, own_w = rows_dev // low, count_t // (pt * low)
    if times_dev != mom or low * moms_dev != tm or own_w * pt * low != count_t:
        raise ValueError("unsupported mesh")
    group = group_rows(half, 16)
    size1 = group if group == 16 else half
    group_h = group_rows(half, 32)
    size3 = group_h if group_h == 32 else half
    dims = (mom, tm, pt, times_dev, moms_dev, rows_dev, points, low, half, own_w, size1, size3, group, group_h)
    mixer = spread_table(cosine_table(count_t), group)
    turner = spread_table(hartley_table(count_k), group_h)
    dma = pltpu.SemaphoreType.DMA
    anywhere = pl.BlockSpec(memory_space=pl.ANY)
    vmem = pl.BlockSpec(memory_space=pltpu.VMEM)
    return pl.pallas_call(
        functools.partial(kernel, dims),
        out_shape=jax.ShapeDtypeStruct((moms_dev, times_dev, bands // pt), F32),
        in_specs=[anywhere, anywhere, vmem, vmem, vmem],
        out_specs=vmem,
        scratch_shapes=[
            pltpu.VMEM((count_t, half, points), BF16),
            pltpu.VMEM((count_t, half, points), BF16),
            pltpu.VMEM((own_w, points, points), BF16),
            pltpu.VMEM((own_w, points, points), BF16),
            pltpu.VMEM((own_w, points, points), BF16),
            pltpu.VMEM((points, points), BF16),
            pltpu.VMEM((count_k, low, half, points), BF16),
            pltpu.VMEM((count_k, rows_dev, points), BF16),
            pltpu.VMEM((count_k, 8, bands), F32),
            pltpu.VMEM((mom * pt, moms_dev, bands // pt), F32),
            pltpu.VMEM((mom * pt, moms_dev, bands // pt), F32),
            dma, dma((half // size1,)), dma, dma, dma, dma,
            dma, dma((half // size3,)), dma, dma((half // size3,)), dma, dma,
        ],
        compiler_params=pltpu.CompilerParams(
            collective_id=0, has_side_effects=True, vmem_limit_bytes=60 << 20),
        name="screened",
    )(chi, green, band, mixer, turner)


def solution(mesh):
    sizes = dict(mesh.shape)
    placed = (P("tm", "mom", "pt", None), P("mom", "tm", "pt", None), P())
    return jax.shard_map(
        functools.partial(local, sizes["mom"], sizes["tm"], sizes["pt"]),
        mesh=mesh, in_specs=placed, out_specs=P("mom", "tm", "pt"), check_vma=False,
    )
```

```python
import functools
import math

import jax
import jax.numpy as jnp
import numpy as np
from jax import lax
from jax.experimental import pallas as pl
from jax.experimental.pallas import tpu as pltpu
from jax.sharding import PartitionSpec as P

COUPLING = 0.8
WINDOW = 3
MESH = pl.DeviceIdType.MESH
BF16, F32 = jnp.bfloat16, jnp.float32


def cosine_table(count):
    index = np.arange(count, dtype=np.float64) + 0.5
    angle = np.pi * index[:, None] * index[None, :] / count
    return (np.sqrt(2.0 / count) * np.cos(angle)).astype(np.float32).astype(BF16)


def hartley_table(count):
    index = np.arange(count, dtype=np.float64)
    angle = 2.0 * np.pi * index[:, None] * index[None, :] / count
    return ((np.cos(angle) + np.sin(angle)) / np.sqrt(count)).astype(np.float32).astype(BF16)


def spread_table(table, rows):
    return jnp.asarray(np.kron(table.astype(np.float32), np.eye(rows, dtype=np.float32)).astype(BF16))


def group_rows(rows, largest):
    size = largest
    while rows % size:
        size //= 2
    return size


def flip(index, bits, count):
    total, place = 0, 1
    while place < count:
        bit = (index // place) % 2
        total = total + place * ((1 - bit) if (bits // place) % 2 else bit)
        place *= 2
    return total


def stacked(value):
    count, rows, width = value.shape
    if rows % 16:
        return value.astype(F32).reshape(count * rows, width).astype(BF16)
    return value.reshape(count * rows, width)


def dot(left, right):
    return jnp.dot(left, right, preferred_element_type=F32)


def kernel(dims, chi, green, band, mixer, turner, out, raw, mix, tiles, four, fourth, square, lat,
           cells, total, part, gathered, send1, recv1, send_g, recv_g, send2, recv2, send3, recv3,
           send4, recv4, send6, recv6, credit_end, credit_mid):
    mom, tm, pt, times_dev, moms_dev, rows_dev, points, low, half, own_w, size1, size3, group, group_h = dims
    m, z, x = lax.axis_index("mom"), lax.axis_index("tm"), lax.axis_index("pt")
    ml, mh = m % low, m // low
    fan = pt * low
    seat = x * low + ml
    count_t = times_dev * tm
    chunks1, chunks3 = half // size1, half // size3
    scale = COUPLING / math.sqrt(points)

    def remote(source, target, send, recv, where):
        return pltpu.make_async_remote_copy(
            src_ref=source, dst_ref=target, send_sem=send, recv_sem=recv,
            device_id=dict(zip(("mom", "tm", "pt"), where)), device_id_type=MESH)

    def await_bytes(ref, sem):
        pltpu.make_async_copy(ref, ref, sem).wait()

    def rows(start, size):
        return pl.ds(pl.multiple_of(start, size), size)

    barrier = pltpu.get_barrier_semaphore()
    greeted = 0
    for i in range(mom):
        for j in range(tm):
            if i or j:
                pl.semaphore_signal(barrier, inc=1, device_id={
                    "mom": flip(m, i, mom), "tm": flip(z, j, tm), "pt": x}, device_id_type=MESH)
                greeted += 1
        for a in range(1, pt):
            pl.semaphore_signal(barrier, inc=1, device_id={
                "mom": flip(m, i, mom), "tm": z, "pt": flip(x, a, pt)}, device_id_type=MESH)
            greeted += 1
    pl.semaphore_wait(barrier, greeted)

    def send_times(c, late):
        kl = 1 - ml if late else ml
        to_z = moms_dev * ml + kl
        for b in range(low):
            to_l = flip(ml, b, low)
            source = chi.at[:, kl, rows(to_l * half + c * size1, size1), :]
            target = raw.at[pl.ds(times_dev * z, times_dev), rows(c * size1, size1), :]
            move = remote(source, target, send1, recv1.at[c], (mh * low + to_l, to_z, x))
            if b:
                move.start()
            else:
                here = to_z == z

                @pl.when(here)
                def _():
                    pltpu.make_async_copy(source, target, recv1.at[c]).start()

                @pl.when(jnp.logical_not(here))
                def _():
                    move.start()

    for i in range(mom):
        to_m = flip(m, i, mom)
        source = green.at[:, to_m]
        target = cells.at[pl.ds(moms_dev * m, moms_dev)]
        if i:
            remote(source, target, send_g, recv_g, (to_m, z, x)).start()
        else:
            pltpu.make_async_copy(source, target, recv_g).start()

    at_end = z % (tm - 1) == 0
    window = min(WINDOW, chunks1)

    def mix_times(c):
        await_bytes(raw.at[:, rows(c * size1, size1), :], recv1.at[c])

        @pl.when(c < chunks1 - window)
        def _():
            for from_z in range(1, tm - 1):
                from_m = mh * low + z // moms_dev
                mine = jnp.logical_and(from_z == z, from_m == m)
                for sem, which in ((credit_end, at_end), (credit_mid, jnp.logical_not(at_end))):
                    @pl.when(jnp.logical_and(which, mine))
                    def _():
                        pl.semaphore_signal(sem.at[ml], inc=1)

                    @pl.when(jnp.logical_and(which, jnp.logical_not(mine)))
                    def _():
                        pl.semaphore_signal(sem.at[ml], inc=1, device_id={
                            "mom": from_m, "tm": from_z, "pt": x}, device_id_type=MESH)

        @pl.loop(0, size1 // group)
        def _(g):
            block = rows(c * size1 + g * group, group)
            mixed = scale * dot(mixer[...], stacked(raw[:, block, :]))
            mix[:, block, :] = mixed.reshape(count_t, group, points).astype(BF16)

        for a in reversed(range(pt)):
            for b in range(low):
                to_x, to_l = flip(x, a, pt), flip(ml, b, low)
                source = mix.at[pl.ds(own_w * (to_x * low + to_l), own_w), rows(c * size1, size1), :]
                target = tiles.at[:, rows(seat * half + c * size1, size1), :]
                if a or b:
                    remote(source, target, send2, recv2, (mh * low + to_l, z, to_x)).start()
                else:
                    pltpu.make_async_copy(source, target, recv2).start()

    @pl.when(at_end)
    def _():
        @pl.loop(0, chunks1)
        def _(c):
            send_times(c, False)

            @pl.when(c % 2 == 1)
            def _():
                send_times(c // 2, True)

        @pl.loop(chunks1 // 2, chunks1)
        def _(c):
            send_times(c, True)

        @pl.loop(0, chunks1)
        def _(c):
            mix_times(c)

    @pl.when(jnp.logical_not(at_end))
    def _():
        def late(c):
            @pl.when(c >= window)
            def _():
                mix_times(c - window)
                for b in range(low):
                    pl.semaphore_wait(credit_mid.at[b], 1)
            send_times(c, True)

        @pl.loop(0, chunks1)
        def _(c):
            @pl.when(c >= window)
            def _():
                for b in range(low):
                    pl.semaphore_wait(credit_end.at[b], 1)
            send_times(c, False)

            @pl.when(c % 2 == 1)
            def _():
                late(c // 2)

        @pl.loop(chunks1 // 2, chunks1)
        def _(c):
            late(c)

        @pl.loop(chunks1 - window, chunks1)
        def _(c):
            mix_times(c)

    await_bytes(tiles, recv2)

    step = points
    while step > 256:
        step //= 2

    @pl.loop(0, own_w)
    def _(w):
        @pl.loop(0, points // step)
        def _(r):
            block = rows(r * step, step)
            square[block, :] = dot(tiles[w, block, :], tiles[w]).astype(BF16)

        @pl.loop(0, points // step)
        def _(r):
            block = rows(r * step, step)
            second = square[block, :]
            two = (tiles[w, block, :].astype(F32) + second.astype(F32)).astype(BF16)
            both = dot(jnp.concatenate([second, two], axis=0), square[...])
            fourth[w, block, :] = both[:step].astype(BF16)
            four[w, block, :] = (two.astype(F32) + both[step:]).astype(BF16)

    @pl.loop(0, chunks3)
    def _(c):
        @pl.loop(0, own_w)
        def _(w):
            if chunks3 == 1:
                left = four[w]
                tiles[w] = (left.astype(F32) + dot(left, fourth[w])).astype(BF16)
            else:
                places = [rows(d * half + c * size3, size3) for d in range(fan)]
                left = jnp.concatenate([four[w, place, :] for place in places], axis=0)
                last = (left.astype(F32) + dot(left, fourth[w])).astype(BF16)
                for d, place in enumerate(places):
                    tiles[w, place, :] = last[d * size3:(d + 1) * size3]

        for a in reversed(range(pt)):
            for b in range(low):
                to_x, to_l = flip(x, a, pt), flip(ml, b, low)
                source = tiles.at[:, rows((to_x * low + to_l) * half + c * size3, size3), :]
                target = raw.at[pl.ds(own_w * seat, own_w), rows(c * size3, size3), :]
                if a or b:
                    remote(source, target, send3, recv3.at[c], (mh * low + to_l, z, to_x)).start()
                else:
                    pltpu.make_async_copy(source, target, recv3.at[c]).start()

    await_bytes(mix.at[pl.ds(0, count_t - own_w)], send2)

    def send_cells(c, j):
        for i in range(mom):
            to_m, to_z = flip(m, i, mom), flip(z, j, tm)
            source = mix.at[times_dev * to_z + to_m, rows(c * size3, size3), :]
            target = lat.at[tm * mh + z, ml, rows(c * size3, size3), :]
            if i or j:
                remote(source, target, send4, recv4.at[c], (to_m, to_z, x)).start()
            else:
                pltpu.make_async_copy(source, target, recv4.at[c]).start()

    @pl.loop(0, chunks3)
    def _(c):
        await_bytes(raw.at[:, rows(c * size3, size3), :], recv3.at[c])

        @pl.loop(0, size3 // group)
        def _(g):
            block = rows(c * size3 + g * group, group)
            timed = dot(mixer[...], stacked(raw[:, block, :]))
            mix[:, block, :] = timed.reshape(count_t, group, points).astype(BF16)

        for j in reversed(range(tm)):
            if j == 1:
                @pl.when(jnp.logical_not(at_end))
                def _():
                    send_cells(c, 1)
            else:
                send_cells(c, j)

    @pl.when(at_end)
    def _():
        @pl.loop(0, chunks3)
        def _(c):
            send_cells(c, 1)

    await_bytes(cells, recv_g)
    total[...] = jnp.zeros_like(total)
    count_k = moms_dev * mom
    bands = band.shape[1]

    @pl.loop(0, chunks3)
    def _(c):
        await_bytes(lat.at[:, :, rows(c * size3, size3), :], recv4.at[c])
        for side in range(low):
            @pl.loop(0, size3 // group_h)
            def _(g):
                block = rows(c * size3 + g * group_h, group_h)
                place = rows(side * half + c * size3 + g * group_h, group_h)
                own = rows(x * rows_dev + side * half + c * size3 + g * group_h, group_h)
                lattice = dot(turner[...], stacked(lat[:, side, block, :]))
                lattice = lattice.reshape(count_k, group_h, points)
                sigma = (cells[:, place, :].astype(F32) * lattice).astype(BF16)
                applied = dot(stacked(sigma), band[...])
                applied = applied.reshape(count_k, group_h, bands) * band[own, :].astype(F32)[None]
                total[...] += jnp.sum(applied.reshape(count_k, group_h // 8, 8, bands), axis=1)

    share = bands // pt
    for to_m in range(mom):
        for to_x in range(pt):
            value = total[pl.ds(moms_dev * to_m, moms_dev), :, pl.ds(to_x * share, share)]
            part[to_m * pt + to_x] = jnp.sum(value, axis=1)
    for i in range(mom):
        for a in range(pt):
            to_m, to_x = flip(m, i, mom), flip(x, a, pt)
            source, target = part.at[to_m * pt + to_x], gathered.at[m * pt + x]
            if i or a:
                remote(source, target, send6, recv6, (to_m, z, to_x)).start()
            else:
                pltpu.make_async_copy(source, target, recv6).start()
    await_bytes(gathered, recv6)
    for t in range(times_dev):
        value = gathered[t * pt]
        for a in range(1, pt):
            value = value + gathered[t * pt + a]
        out[:, t, :] = value

    stays = z // moms_dev == ml

    @pl.when(stays)
    def _():
        await_bytes(chi.at[pl.ds(0, times_dev - times_dev // (low * moms_dev))], send1)

    @pl.when(jnp.logical_not(stays))
    def _():
        await_bytes(chi, send1)

    await_bytes(green.at[:, pl.ds(0, mom - 1)], send_g)
    await_bytes(mix.at[pl.ds(0, count_t - own_w)], send3)
    await_bytes(mix.at[pl.ds(0, count_t - 1)], send4)
    await_bytes(part.at[pl.ds(0, mom * pt - 1)], send6)


def local(mom, tm, pt, chi, green, band):
    times_dev, moms_dev, rows_dev, points = chi.shape
    bands = band.shape[1]
    count_t, count_k = times_dev * tm, moms_dev * mom
    low = tm // moms_dev
    half, own_w = rows_dev // low, count_t // (pt * low)
    if times_dev != mom or low != 2 or low * moms_dev != tm or own_w * pt * low != count_t:
        raise ValueError("unsupported mesh")
    group = group_rows(half, 16)
    size1 = group if group == 16 else half
    group_h = group_rows(half, 32)
    size3 = group_h if group_h == 32 else half
    dims = (mom, tm, pt, times_dev, moms_dev, rows_dev, points, low, half, own_w, size1, size3, group, group_h)
    mixer = spread_table(cosine_table(count_t), group)
    turner = spread_table(hartley_table(count_k), group_h)
    dma = pltpu.SemaphoreType.DMA
    anywhere = pl.BlockSpec(memory_space=pl.ANY)
    vmem = pl.BlockSpec(memory_space=pltpu.VMEM)
    return pl.pallas_call(
        functools.partial(kernel, dims),
        out_shape=jax.ShapeDtypeStruct((moms_dev, times_dev, bands // pt), F32),
        in_specs=[anywhere, anywhere, vmem, vmem, vmem],
        out_specs=vmem,
        scratch_shapes=[
            pltpu.VMEM((count_t, half, points), BF16),
            pltpu.VMEM((count_t, half, points), BF16),
            pltpu.VMEM((own_w, points, points), BF16),
            pltpu.VMEM((own_w, points, points), BF16),
            pltpu.VMEM((own_w, points, points), BF16),
            pltpu.VMEM((points, points), BF16),
            pltpu.VMEM((count_k, low, half, points), BF16),
            pltpu.VMEM((count_k, rows_dev, points), BF16),
            pltpu.VMEM((count_k, 8, bands), F32),
            pltpu.VMEM((mom * pt, moms_dev, bands // pt), F32),
            pltpu.VMEM((mom * pt, moms_dev, bands // pt), F32),
            dma, dma((half // size1,)), dma, dma, dma, dma,
            dma, dma((half // size3,)), dma, dma((half // size3,)), dma, dma,
            pltpu.SemaphoreType.REGULAR((low,)), pltpu.SemaphoreType.REGULAR((low,)),
        ],
        compiler_params=pltpu.CompilerParams(
            collective_id=0, has_side_effects=True, vmem_limit_bytes=60 << 20),
        name="screened",
    )(chi, green, band, mixer, turner)


def solution(mesh):
    sizes = dict(mesh.shape)
    placed = (P("tm", "mom", "pt", None), P("mom", "tm", "pt", None), P())
    return jax.shard_map(
        functools.partial(local, sizes["mom"], sizes["tm"], sizes["pt"]),
        mesh=mesh, in_specs=placed, out_specs=P("mom", "tm", "pt"), check_vma=False,
    )
```

```python
import functools
import math

import jax
import jax.numpy as jnp
import numpy as np
from jax import lax
from jax.experimental import pallas as pl
from jax.experimental.pallas import tpu as pltpu
from jax.sharding import PartitionSpec as P

COUPLING = 0.8
WINDOW = 3
MESH = pl.DeviceIdType.MESH
BF16, F32 = jnp.bfloat16, jnp.float32


def cosine_table(count):
    index = np.arange(count, dtype=np.float64) + 0.5
    angle = np.pi * index[:, None] * index[None, :] / count
    return (np.sqrt(2.0 / count) * np.cos(angle)).astype(np.float32).astype(BF16)


def hartley_table(count):
    index = np.arange(count, dtype=np.float64)
    angle = 2.0 * np.pi * index[:, None] * index[None, :] / count
    return ((np.cos(angle) + np.sin(angle)) / np.sqrt(count)).astype(np.float32).astype(BF16)


def spread_table(table, rows):
    return jnp.asarray(np.kron(table.astype(np.float32), np.eye(rows, dtype=np.float32)).astype(BF16))


def group_rows(rows, largest):
    size = largest
    while rows % size:
        size //= 2
    return size


def flip(index, bits, count):
    total, place = 0, 1
    while place < count:
        bit = (index // place) % 2
        total = total + place * ((1 - bit) if (bits // place) % 2 else bit)
        place *= 2
    return total


def stacked(value):
    count, rows, width = value.shape
    if rows % 16:
        return value.astype(F32).reshape(count * rows, width).astype(BF16)
    return value.reshape(count * rows, width)


def dot(left, right):
    return jnp.dot(left, right, preferred_element_type=F32)


def kernel(dims, chi, green, band, mixer, turner, out, raw, mix, tiles, four, fourth, square, lat,
           cells, total, part, gathered, send1, recv1, send_g, recv_g, send2, recv2, send3, recv3,
           send4, recv4, send6, recv6, credit_end, credit_mid):
    mom, tm, pt, times_dev, moms_dev, rows_dev, points, low, half, own_w, size1, size3, group, group_h = dims
    m, z, x = lax.axis_index("mom"), lax.axis_index("tm"), lax.axis_index("pt")
    ml, mh = m % low, m // low
    fan = pt * low
    seat = x * low + ml
    count_t = times_dev * tm
    chunks1, chunks3 = half // size1, half // size3
    scale = COUPLING / math.sqrt(points)

    def remote(source, target, send, recv, where):
        return pltpu.make_async_remote_copy(
            src_ref=source, dst_ref=target, send_sem=send, recv_sem=recv,
            device_id=dict(zip(("mom", "tm", "pt"), where)), device_id_type=MESH)

    def await_bytes(ref, sem):
        pltpu.make_async_copy(ref, ref, sem).wait()

    def rows(start, size):
        return pl.ds(pl.multiple_of(start, size), size)

    barrier = pltpu.get_barrier_semaphore()
    greeted = 0
    for i in range(mom):
        for j in range(tm):
            if i or j:
                pl.semaphore_signal(barrier, inc=1, device_id={
                    "mom": flip(m, i, mom), "tm": flip(z, j, tm), "pt": x}, device_id_type=MESH)
                greeted += 1
        for a in range(1, pt):
            pl.semaphore_signal(barrier, inc=1, device_id={
                "mom": flip(m, i, mom), "tm": z, "pt": flip(x, a, pt)}, device_id_type=MESH)
            greeted += 1
    pl.semaphore_wait(barrier, greeted)

    def send_times(c, late):
        kl = 1 - ml if late else ml
        to_z = moms_dev * ml + kl
        for b in range(low):
            to_l = flip(ml, b, low)
            source = chi.at[:, kl, rows(to_l * half + c * size1, size1), :]
            target = raw.at[pl.ds(times_dev * z, times_dev), rows(c * size1, size1), :]
            move = remote(source, target, send1, recv1.at[c], (mh * low + to_l, to_z, x))
            if b:
                move.start()
            else:
                here = to_z == z

                @pl.when(here)
                def _():
                    pltpu.make_async_copy(source, target, recv1.at[c]).start()

                @pl.when(jnp.logical_not(here))
                def _():
                    move.start()

    for i in range(mom):
        to_m = flip(m, i, mom)
        source = green.at[:, to_m]
        target = cells.at[pl.ds(moms_dev * m, moms_dev)]
        if i:
            remote(source, target, send_g, recv_g, (to_m, z, x)).start()
        else:
            pltpu.make_async_copy(source, target, recv_g).start()

    at_end = z % (tm - 1) == 0
    window = min(WINDOW, chunks1)

    def mix_times(c):
        await_bytes(raw.at[:, rows(c * size1, size1), :], recv1.at[c])

        @pl.when(c < chunks1 - window)
        def _():
            for from_z in range(1, tm - 1):
                from_m = mh * low + z // moms_dev
                mine = jnp.logical_and(from_z == z, from_m == m)
                for sem, which in ((credit_end, at_end), (credit_mid, jnp.logical_not(at_end))):
                    @pl.when(jnp.logical_and(which, mine))
                    def _():
                        pl.semaphore_signal(sem.at[ml], inc=1)

                    @pl.when(jnp.logical_and(which, jnp.logical_not(mine)))
                    def _():
                        pl.semaphore_signal(sem.at[ml], inc=1, device_id={
                            "mom": from_m, "tm": from_z, "pt": x}, device_id_type=MESH)

        @pl.loop(0, size1 // group)
        def _(g):
            block = rows(c * size1 + g * group, group)
            mixed = scale * dot(mixer[...], stacked(raw[:, block, :]))
            mix[:, block, :] = mixed.reshape(count_t, group, points).astype(BF16)

        for a in reversed(range(pt)):
            for b in range(low):
                to_x, to_l = flip(x, a, pt), flip(ml, b, low)
                source = mix.at[pl.ds(own_w * (to_x * low + to_l), own_w), rows(c * size1, size1), :]
                target = tiles.at[:, rows(seat * half + c * size1, size1), :]
                if a or b:
                    remote(source, target, send2, recv2, (mh * low + to_l, z, to_x)).start()
                else:
                    pltpu.make_async_copy(source, target, recv2).start()

    @pl.when(at_end)
    def _():
        @pl.loop(0, chunks1)
        def _(c):
            send_times(c, False)

            @pl.when(c % 2 == 1)
            def _():
                send_times(c // 2, True)

        @pl.loop(chunks1 // 2, chunks1)
        def _(c):
            send_times(c, True)

        @pl.loop(0, chunks1)
        def _(c):
            mix_times(c)

    @pl.when(jnp.logical_not(at_end))
    def _():
        def late(c):
            @pl.when(c >= window)
            def _():
                mix_times(c - window)
                for b in range(low):
                    pl.semaphore_wait(credit_mid.at[b], 1)
            send_times(c, True)

        @pl.loop(0, chunks1)
        def _(c):
            @pl.when(c >= window)
            def _():
                for b in range(low):
                    pl.semaphore_wait(credit_end.at[b], 1)
            send_times(c, False)

            @pl.when(c % 2 == 1)
            def _():
                late(c // 2)

        @pl.loop(chunks1 // 2, chunks1)
        def _(c):
            late(c)

        @pl.loop(chunks1 - window, chunks1)
        def _(c):
            mix_times(c)

    await_bytes(tiles, recv2)

    step = points
    while step > 512:
        step //= 2

    @pl.loop(0, own_w)
    def _(w):
        @pl.loop(0, points // step)
        def _(r):
            block = rows(r * step, step)
            square[block, :] = dot(tiles[w, block, :], tiles[w]).astype(BF16)

        @pl.loop(0, points // step)
        def _(r):
            block = rows(r * step, step)
            second = square[block, :]
            two = (tiles[w, block, :].astype(F32) + second.astype(F32)).astype(BF16)
            both = dot(jnp.concatenate([second, two], axis=0), square[...])
            fourth[w, block, :] = both[:step].astype(BF16)
            four[w, block, :] = (two.astype(F32) + both[step:]).astype(BF16)

    @pl.loop(0, chunks3)
    def _(c):
        @pl.loop(0, own_w)
        def _(w):
            if chunks3 == 1:
                left = four[w]
                tiles[w] = (left.astype(F32) + dot(left, fourth[w])).astype(BF16)
            else:
                places = [rows(d * half + c * size3, size3) for d in range(fan)]
                left = jnp.concatenate([four[w, place, :] for place in places], axis=0)
                last = (left.astype(F32) + dot(left, fourth[w])).astype(BF16)
                for d, place in enumerate(places):
                    tiles[w, place, :] = last[d * size3:(d + 1) * size3]

        for a in reversed(range(pt)):
            for b in range(low):
                to_x, to_l = flip(x, a, pt), flip(ml, b, low)
                source = tiles.at[:, rows((to_x * low + to_l) * half + c * size3, size3), :]
                target = raw.at[pl.ds(own_w * seat, own_w), rows(c * size3, size3), :]
                if a or b:
                    remote(source, target, send3, recv3.at[c], (mh * low + to_l, z, to_x)).start()
                else:
                    pltpu.make_async_copy(source, target, recv3.at[c]).start()

    await_bytes(mix.at[pl.ds(0, count_t - own_w)], send2)

    def send_cells(c, j):
        for i in range(mom):
            to_m, to_z = flip(m, i, mom), flip(z, j, tm)
            source = mix.at[times_dev * to_z + to_m, rows(c * size3, size3), :]
            target = lat.at[tm * mh + z, ml, rows(c * size3, size3), :]
            if i or j:
                remote(source, target, send4, recv4.at[c], (to_m, to_z, x)).start()
            else:
                pltpu.make_async_copy(source, target, recv4.at[c]).start()

    @pl.loop(0, chunks3)
    def _(c):
        await_bytes(raw.at[:, rows(c * size3, size3), :], recv3.at[c])

        @pl.loop(0, size3 // group)
        def _(g):
            block = rows(c * size3 + g * group, group)
            timed = dot(mixer[...], stacked(raw[:, block, :]))
            mix[:, block, :] = timed.reshape(count_t, group, points).astype(BF16)

        for j in reversed(range(tm)):
            if j == 1:
                @pl.when(jnp.logical_not(at_end))
                def _():
                    send_cells(c, 1)
            else:
                send_cells(c, j)

    @pl.when(at_end)
    def _():
        @pl.loop(0, chunks3)
        def _(c):
            send_cells(c, 1)

    await_bytes(cells, recv_g)
    total[...] = jnp.zeros_like(total)
    count_k = moms_dev * mom
    bands = band.shape[1]

    @pl.loop(0, chunks3)
    def _(c):
        await_bytes(lat.at[:, :, rows(c * size3, size3), :], recv4.at[c])
        for side in range(low):
            @pl.loop(0, size3 // group_h)
            def _(g):
                block = rows(c * size3 + g * group_h, group_h)
                place = rows(side * half + c * size3 + g * group_h, group_h)
                own = rows(x * rows_dev + side * half + c * size3 + g * group_h, group_h)
                lattice = dot(turner[...], stacked(lat[:, side, block, :]))
                lattice = lattice.reshape(count_k, group_h, points)
                sigma = (cells[:, place, :].astype(F32) * lattice).astype(BF16)
                applied = dot(stacked(sigma), band[...])
                applied = applied.reshape(count_k, group_h, bands) * band[own, :].astype(F32)[None]
                total[...] += jnp.sum(applied.reshape(count_k, group_h // 8, 8, bands), axis=1)

    share = bands // pt
    for to_m in range(mom):
        for to_x in range(pt):
            value = total[pl.ds(moms_dev * to_m, moms_dev), :, pl.ds(to_x * share, share)]
            part[to_m * pt + to_x] = jnp.sum(value, axis=1)
    for i in range(mom):
        for a in range(pt):
            to_m, to_x = flip(m, i, mom), flip(x, a, pt)
            source, target = part.at[to_m * pt + to_x], gathered.at[m * pt + x]
            if i or a:
                remote(source, target, send6, recv6, (to_m, z, to_x)).start()
            else:
                pltpu.make_async_copy(source, target, recv6).start()
    await_bytes(gathered, recv6)
    for t in range(times_dev):
        value = gathered[t * pt]
        for a in range(1, pt):
            value = value + gathered[t * pt + a]
        out[:, t, :] = value

    stays = z // moms_dev == ml

    @pl.when(stays)
    def _():
        await_bytes(chi.at[pl.ds(0, times_dev - times_dev // (low * moms_dev))], send1)

    @pl.when(jnp.logical_not(stays))
    def _():
        await_bytes(chi, send1)

    await_bytes(green.at[:, pl.ds(0, mom - 1)], send_g)
    await_bytes(mix.at[pl.ds(0, count_t - own_w)], send3)
    await_bytes(mix.at[pl.ds(0, count_t - 1)], send4)
    await_bytes(part.at[pl.ds(0, mom * pt - 1)], send6)


def local(mom, tm, pt, chi, green, band):
    times_dev, moms_dev, rows_dev, points = chi.shape
    bands = band.shape[1]
    count_t, count_k = times_dev * tm, moms_dev * mom
    low = tm // moms_dev
    half, own_w = rows_dev // low, count_t // (pt * low)
    if times_dev != mom or low != 2 or low * moms_dev != tm or own_w * pt * low != count_t:
        raise ValueError("unsupported mesh")
    group = group_rows(half, 16)
    size1 = group if group == 16 else half
    group_h = group_rows(half, 32)
    size3 = group_h if group_h == 32 else half
    dims = (mom, tm, pt, times_dev, moms_dev, rows_dev, points, low, half, own_w, size1, size3, group, group_h)
    mixer = spread_table(cosine_table(count_t), group)
    turner = spread_table(hartley_table(count_k), group_h)
    dma = pltpu.SemaphoreType.DMA
    anywhere = pl.BlockSpec(memory_space=pl.ANY)
    vmem = pl.BlockSpec(memory_space=pltpu.VMEM)
    return pl.pallas_call(
        functools.partial(kernel, dims),
        out_shape=jax.ShapeDtypeStruct((moms_dev, times_dev, bands // pt), F32),
        in_specs=[anywhere, anywhere, vmem, vmem, vmem],
        out_specs=vmem,
        scratch_shapes=[
            pltpu.VMEM((count_t, half, points), BF16),
            pltpu.VMEM((count_t, half, points), BF16),
            pltpu.VMEM((own_w, points, points), BF16),
            pltpu.VMEM((own_w, points, points), BF16),
            pltpu.VMEM((own_w, points, points), BF16),
            pltpu.VMEM((points, points), BF16),
            pltpu.VMEM((count_k, low, half, points), BF16),
            pltpu.VMEM((count_k, rows_dev, points), BF16),
            pltpu.VMEM((count_k, 8, bands), F32),
            pltpu.VMEM((mom * pt, moms_dev, bands // pt), F32),
            pltpu.VMEM((mom * pt, moms_dev, bands // pt), F32),
            dma, dma((half // size1,)), dma, dma, dma, dma,
            dma, dma((half // size3,)), dma, dma((half // size3,)), dma, dma,
            pltpu.SemaphoreType.REGULAR((low,)), pltpu.SemaphoreType.REGULAR((low,)),
        ],
        compiler_params=pltpu.CompilerParams(
            collective_id=0, has_side_effects=True, vmem_limit_bytes=60 << 20),
        name="screened",
    )(chi, green, band, mixer, turner)


def solution(mesh):
    sizes = dict(mesh.shape)
    placed = (P("tm", "mom", "pt", None), P("mom", "tm", "pt", None), P())
    return jax.shard_map(
        functools.partial(local, sizes["mom"], sizes["tm"], sizes["pt"]),
        mesh=mesh, in_specs=placed, out_specs=P("mom", "tm", "pt"), check_vma=False,
    )
```
